1024 devices in a mesh: dp: 16 (over x_lo, y), seq: 64 (over z, x_hi, core).
Axes of the slice: x: 4 (x_hi: 2, x_lo: 2; x = x_hi * 2 + x_lo), y: 8, z: 16, core: 2. Of those that a mesh axis runs over, the one named last changes fastest.
Arguments:
- cotangent: bfloat16 [16, 64, 128, 1152], P('dp', None, 'seq'), may hold values from -6 to 6
- query_time: bfloat16 [16, 64, 128, 576], P('dp', None, 'seq'), may hold values from -6 to 6
- key_time: bfloat16 [16, 64, 128, 576], P('dp', None, 'seq'), may hold values from -6 to 6
- value_time: bfloat16 [16, 64, 128, 576], P('dp', None, 'seq'), may hold values from -6 to 6
- query_space: bfloat16 [16, 64, 128, 576], P('dp', 'seq'), may hold values from -6 to 6
- key_space: bfloat16 [16, 64, 128, 576], P('dp', 'seq'), may hold values from -6 to 6
- value_space: bfloat16 [16, 64, 128, 576], P('dp', 'seq'), may hold values from -6 to 6
- weight_time: bfloat16 [1152, 576], replicated, may hold values from -0.25 to 0.25
- weight_space: bfloat16 [1152, 576], replicated, may hold values from -0.25 to 0.25
- gate_time: float32 [16, 1152], P('dp'), may hold values from 0.25 to 2
- gate_space: float32 [16, 1152], P('dp'), may hold values from 0.25 to 2
Outputs:
- query_grad_time: bfloat16 [16, 64, 128, 576], P('dp', None, 'seq')
- key_grad_time: bfloat16 [16, 64, 128, 576], P('dp', None, 'seq')
- value_grad_time: bfloat16 [16, 64, 128, 576], P('dp', None, 'seq')
- query_grad_space: bfloat16 [16, 64, 128, 576], P('dp', 'seq')
- key_grad_space: bfloat16 [16, 64, 128, 576], P('dp', 'seq')
- value_grad_space: bfloat16 [16, 64, 128, 576], P('dp', 'seq')
- weight_grad_time: float32 [1152, 576], P('seq', 'dp')
- gate_grad_time: float32 [16, 1152], P('dp')
- gate_grad_space: float32 [16, 1152], P('dp')
The draws below stay inside these ranges and needn't reach their ends.
All inputs are finite; a program needn't handle non-finite values.
Results may differ from the reference program's by a relative error of at most 0.035.
Values may be sent and summed in bfloat16 or wider, within the bound.
No kernel may reach another device: no remote copies, remote signals or barrier semaphores. Data moves between devices by JAX's collectives and lax.ppermute only.
A program may use at most 32 MiB of HBM per device.

```python
import math
import jax
import jax.numpy as jnp
from jax import lax

D = 1152
HEAD_DIM = 72
HEADS = 8
POSITIONS = 128
ATTN = 576
FRAMES = 64
CLIPS = 16
N_SEQ = 64


def drawn_pair(key, stream):
    width = HEADS * HEAD_DIM
    full_shape = (CLIPS, FRAMES, POSITIONS, width)
    queries = jnp.clip(jax.random.normal(jax.random.fold_in(key, stream), full_shape, jnp.float32), -6.0, 6.0)
    key_rows = jnp.clip(jax.random.normal(jax.random.fold_in(key, stream + 1), full_shape, jnp.float32), -6.0, 6.0)
    return (queries, key_rows)


def draw_query_time(key, part):
    return drawn_pair(key, 10)[0].astype(jnp.bfloat16)


def draw_key_time(key, part):
    return drawn_pair(key, 10)[1].astype(jnp.bfloat16)


def draw_query_space(key, part):
    return drawn_pair(key, 30)[0].astype(jnp.bfloat16)


def draw_key_space(key, part):
    return drawn_pair(key, 30)[1].astype(jnp.bfloat16)


def block_levels(rng, dims, split, low, top_value):
    def one(axis_at, shards_of):
        steps = jax.random.uniform(jax.random.fold_in(jax.random.fold_in(rng, 6), axis_at), (shards_of,), jnp.float32, low / len(split), top_value / len(split))
        return jnp.repeat(jnp.exp(steps), dims[axis_at] // shards_of).reshape((-1,) + (1,) * (len(dims) - axis_at - 1))

    level = one(*split[0])
    for cut in split[1:]:
        level = level * one(*cut)
    return level


def noise(own_key, dims, spread, reach, cuts=(), dtype=jnp.bfloat16):
    level = block_levels(own_key, dims, cuts, -0.22, 0.18) if cuts else 1.0
    drawn = jax.random.normal(own_key, dims, jnp.float32) * spread * level
    return jnp.minimum(jnp.maximum(drawn, -reach), reach).astype(dtype)


def setup_inputs(seed: int = 0) -> dict:
    arg_keys = jax.random.split(jax.random.key(seed), 12)
    return {
        "cotangent": noise(arg_keys[0], (CLIPS, FRAMES, POSITIONS, D), 1.0, 6.0, ((0, 16), (2, 64))),
        "query_time": draw_query_time(jax.random.fold_in(arg_keys[11], 71), 0),
        "key_time": draw_key_time(jax.random.fold_in(arg_keys[11], 71), 0),
        "value_time": noise(arg_keys[3], (CLIPS, FRAMES, POSITIONS, ATTN), 1.0, 6.0, ((0, 16), (2, 64))),
        "query_space": draw_query_space(jax.random.fold_in(arg_keys[11], 71), 0),
        "key_space": draw_key_space(jax.random.fold_in(arg_keys[11], 71), 0),
        "value_space": noise(arg_keys[6], (CLIPS, FRAMES, POSITIONS, ATTN), 1.0, 6.0, ((0, 16), (1, 64))),
        "weight_time": noise(arg_keys[7], (D, ATTN), ATTN ** -0.5, 0.25),
        "weight_space": noise(arg_keys[8], (D, ATTN), ATTN ** -0.5, 0.25),
        "gate_time": jnp.clip(0.25 + 1.75 * jax.random.uniform(arg_keys[9], (CLIPS, D), jnp.float32) ** block_levels(arg_keys[9], (CLIPS, D), ((0, 16),), -0.2, 0.2), 0.25, 2.0),
        "gate_space": jnp.clip(0.25 + 1.75 * jax.random.uniform(arg_keys[10], (CLIPS, D), jnp.float32) ** block_levels(arg_keys[10], (CLIPS, D), ((0, 16),), -0.2, 0.2), 0.25, 2.0),
    }


def block_back(grad_tok, query, key_rows, value_rows, weight, gate, over_first):
    if over_first:
        tok_query, tok_key = ('ixhd', 'jxhd')
    else:
        tok_query, tok_key = ('xihd', 'xjhd')
    high = lax.Precision.HIGHEST
    head_shape = query.shape[:2] + (HEADS, HEAD_DIM)
    width = weight.shape[1]
    model_width = weight.shape[0]
    score_scale = 1.0 / math.sqrt(HEAD_DIM)
    query_heads = query.reshape(head_shape).astype(jnp.float32)
    key_heads = key_rows.reshape(head_shape).astype(jnp.float32)
    value_heads = value_rows.reshape(head_shape).astype(jnp.float32)
    scores = jnp.einsum(tok_query + ',' + tok_key + '->xhij', query_heads, key_heads, precision=high) * score_scale
    probs = jax.nn.softmax(scores, axis=-1)
    probs_low = probs.astype(jnp.bfloat16)
    attended = jnp.einsum('xhij,' + tok_key + '->' + tok_query, probs_low.astype(jnp.float32), value_heads, precision=high).astype(jnp.bfloat16)
    flat_out = attended.reshape(-1, width)
    flat_grad = grad_tok.reshape(-1, model_width)
    gated_grad = (gate * flat_grad.astype(jnp.float32)).astype(jnp.bfloat16)
    d_attended = jnp.dot(gated_grad, weight, preferred_element_type=jnp.float32).astype(jnp.bfloat16)
    projected = jnp.dot(flat_out, weight.T, preferred_element_type=jnp.float32)
    gate_part = lax.optimization_barrier(jnp.sum(flat_grad.astype(jnp.float32) * projected, axis=0))
    d_heads = d_attended.reshape(head_shape).astype(jnp.float32)
    attended_heads = attended.astype(jnp.float32)
    d_probs = jnp.einsum(tok_query + ',' + tok_key + '->xhij', d_heads, value_heads, precision=high)
    row_delta = jnp.einsum(tok_query + ',' + tok_query + '->xhi', d_heads, attended_heads, precision=high)
    d_scores = (probs * (d_probs - row_delta[..., None])).astype(jnp.bfloat16).astype(jnp.float32)
    grad_query = jnp.einsum('xhij,' + tok_key + '->' + tok_query, d_scores, key_heads, precision=high) * score_scale
    grad_key = jnp.einsum('xhij,' + tok_query + '->' + tok_key, d_scores, query_heads, precision=high) * score_scale
    grad_value = jnp.einsum('xhij,' + tok_query + '->' + tok_key, probs_low.astype(jnp.float32), d_heads, precision=high)
    return (grad_query.astype(jnp.bfloat16).reshape(query.shape), grad_key.astype(jnp.bfloat16).reshape(query.shape), grad_value.astype(jnp.bfloat16).reshape(query.shape), gated_grad, flat_out, gate_part)

def reference(cotangent, query_time, key_time, value_time, query_space, key_space, value_space, weight_time, weight_space, gate_time, gate_space):
    norm_weight = 1.0 / math.sqrt(CLIPS * FRAMES * POSITIONS)
    norm_gate = 1.0 / math.sqrt(FRAMES * POSITIONS)
    block_len = POSITIONS // N_SEQ

    def one_clip(clip_items):
        grad_tok, q_tm, k_tm, v_tm, q_sp, k_sp, v_sp, g_tm, g_sp = clip_items
        timed = block_back(grad_tok, q_tm, k_tm, v_tm, weight_time, g_tm, True)
        spaced = block_back(grad_tok, q_sp, k_sp, v_sp, weight_space, g_sp, False)
        gated_blocks = timed[3].reshape(FRAMES, N_SEQ, block_len, D).transpose(1, 0, 2, 3).reshape(N_SEQ, FRAMES * block_len, D)
        out_blocks = timed[4].reshape(FRAMES, N_SEQ, block_len, ATTN).transpose(1, 0, 2, 3).reshape(N_SEQ, FRAMES * block_len, ATTN)

        def add_block(total, pair):
            gated_part, out_part = pair
            term = jnp.dot(gated_part.T, out_part, preferred_element_type=jnp.float32) * norm_weight
            low = lax.optimization_barrier(term.astype(jnp.bfloat16))
            return (total + low.astype(jnp.float32), None)
        weight_sum, unused = lax.scan(add_block, jnp.zeros((D, ATTN), jnp.float32), (gated_blocks, out_blocks))
        return (timed[0], timed[1], timed[2], spaced[0], spaced[1], spaced[2], weight_sum, timed[5], spaced[5])
    per_clip = lax.map(one_clip, (cotangent, query_time, key_time, value_time, query_space, key_space, value_space, gate_time, gate_space))
    weight_grad_time = lax.optimization_barrier(jnp.sum(per_clip[6], axis=0))
    return (per_clip[0], per_clip[1], per_clip[2], per_clip[3], per_clip[4], per_clip[5], weight_grad_time, per_clip[7] * norm_gate, per_clip[8] * norm_gate)
```

```python
import functools
import math

import jax
import jax.numpy as jnp
import numpy as np
from jax import lax
from jax.experimental import pallas as pl
from jax.experimental.pallas import tpu as pltpu
from jax.sharding import Mesh
from jax.sharding import PartitionSpec as P

HD = 72
HEADS = 8
WIDTH = 576
MODEL = 1152
TOK = 128
NT = (((1,), (1,)), ((), ()))
TN = (((0,), (0,)), ((), ()))
NN = (((1,), (0,)), ((), ()))
F32 = jnp.float32
BF16 = jnp.bfloat16
DP = ("xl", "y")
SEQ = ("z", "xh", "c")
ROWS = ("z", "xh")
SCALE = 1.0 / math.sqrt(HD)


def dot(a, b, dims):
    return lax.dot_general(a, b, dims, preferred_element_type=F32)


def probs_of(key, query, keep):
    scores = dot(key, query, TN) * SCALE
    if keep is not None:
        scores = jnp.where(keep, scores, -jnp.inf)
    top = jnp.max(scores, axis=0, keepdims=True)
    e = jnp.exp(scores - top)
    return e / jnp.sum(e, axis=0, keepdims=True)


def same_position():
    i = lax.broadcasted_iota(jnp.int32, (TOK, TOK), 0)
    j = lax.broadcasted_iota(jnp.int32, (TOK, TOK), 1)
    return ((i + j) & 1) == 0


def turned(x):
    return x.astype(F32).T.astype(BF16)


def rows_of(ref, h):
    return ref[h * HD : (h + 1) * HD, :]


def forward_kernel(over_time, q_ref, k_ref, v_ref, out_ref, *turned_refs):
    keep = same_position() if over_time else None
    if over_time:
        for src, dst in zip((q_ref, k_ref, v_ref), turned_refs):
            dst[...] = turned(src[...])
        q_ref, k_ref, v_ref = turned_refs
    for h in range(HEADS):
        low = probs_of(rows_of(k_ref, h), rows_of(q_ref, h), keep).astype(BF16)
        out_ref[h * HD : (h + 1) * HD, :] = dot(rows_of(v_ref, h), low, NN).astype(BF16)


def project_kernel(cot_ref, gate_ref, w_ref, att_ref, d_ref, part_ref):
    cot = cot_ref[...].astype(F32)
    gated = (cot * gate_ref[...]).astype(BF16)
    d_ref[...] = dot(w_ref[...], gated, NT).astype(BF16)
    projected = dot(att_ref[...], w_ref[...], TN)
    part_ref[...] = jnp.sum(cot * projected, axis=0, keepdims=True)


def backward_kernel(over_time, q_ref, k_ref, v_ref, att_ref, d_ref, gq_ref, gk_ref, gv_ref, *scratch):
    keep = same_position() if over_time else None
    outs = scratch if over_time else (gq_ref, gk_ref, gv_ref)
    for h in range(HEADS):
        sl = slice(h * HD, (h + 1) * HD)
        q, k, v, a, d = (rows_of(r, h) for r in (q_ref, k_ref, v_ref, att_ref, d_ref))
        probs = probs_of(k, q, keep)
        low = probs.astype(BF16)
        d_probs = dot(v, d, TN)
        delta = jnp.sum(d.astype(F32) * a.astype(F32), axis=0, keepdims=True)
        d_scores = (probs * (d_probs - delta)).astype(BF16)
        grads = (dot(k, d_scores, NN) * SCALE, dot(q, d_scores, NT) * SCALE, dot(d, low, NT))
        for ref, g in zip(outs, grads):
            ref[sl, :] = g.astype(ref.dtype)
    if over_time:
        for src, dst in zip(scratch, (gq_ref, gk_ref, gv_ref)):
            dst[...] = src[...].T.astype(BF16)


def select_kernel(core_ref, own_ref, other_ref, gate_ref, out_ref):
    core = core_ref[0]
    row = lax.broadcasted_iota(jnp.int32, (WIDTH, 1), 0)
    block = (row * 3641) >> 16
    channel = row + 18 * (block + core)
    col = lax.broadcasted_iota(jnp.int32, (WIDTH, MODEL), 1)
    pick = jnp.where(col == channel, 1.0, 0.0).astype(BF16)
    for i, ref in enumerate((own_ref, other_ref)):
        gated = (ref[...].astype(F32) * gate_ref[...]).astype(BF16)
        out_ref[:, i * TOK : (i + 1) * TOK] = dot(pick, gated, NT).astype(BF16)


def product_kernel(norm, half_ref, own_ref, other_ref, sel_ref, keep_ref, send_ref):
    half = half_ref[0]
    sel = sel_ref[...]
    for ref, index in ((keep_ref, half), (send_ref, 1 - half)):
        rows = pl.ds(pl.multiple_of(index * 288, 32), 288)
        att = jnp.concatenate([own_ref[rows, :], other_ref[rows, :]], axis=1)
        ref[...] = (dot(att, sel, NT) * norm).astype(ref.dtype)


def join_kernel(keep_ref, came_ref, out_ref):
    total = (keep_ref[...] + came_ref[...].astype(F32)).astype(BF16)
    out_ref[...] = total.reshape(out_ref.shape)


def pack_kernel(core_ref, in_ref, time_ref, space_ref, came_ref, out_ref):
    total = jnp.sum(in_ref[...].astype(F32), axis=0)
    total = jnp.concatenate([total, jnp.zeros((4, WIDTH), F32)], axis=0)
    gate = jnp.where(core_ref[0] == 0, time_ref[...], space_ref[...]) + came_ref[...]
    last = gate[:, 1024:]
    tail = jnp.concatenate([last[:, 16 * a : 16 * a + 16] for a in range(8)], axis=0)
    gap = jnp.zeros((8, 22), F32)
    low = jnp.concatenate([gate[:, 128 * a : 128 * a + 128] for a in range(8)], axis=0)
    for m in range(32):
        parts = [total[8 * b : 8 * b + 8, 18 * m : 18 * m + 18] for b in range(5)]
        high = jnp.concatenate(parts + [gap, tail], axis=1)
        out_ref[m] = jnp.concatenate([high, low], axis=0).astype(BF16)


def finish_kernel(norm, in_ref, out_ref, gate_ref):
    total = jnp.sum(in_ref[...].astype(F32), axis=0)
    high = total[:8]
    flipped = high.T
    for b in range(5):
        n = 8 if b < 4 else 4
        out_ref[:, 8 * b : 8 * b + n] = flipped[18 * b : 18 * b + 18, :n]
    for a in range(8):
        gate_ref[:, 128 * a : 128 * a + 128] = total[8 + a : 9 + a, :] * norm
    last = jnp.concatenate([high[a : a + 1, 112:] for a in range(8)], axis=1)
    gate_ref[:, 1024:] = last * norm


def call(kernel, outs, *args, scratch=(), flops=0, scalars=0):
    specs = [pl.BlockSpec(memory_space=pltpu.SMEM)] * scalars
    specs += [pl.BlockSpec(memory_space=pltpu.VMEM)] * (len(args) - scalars)
    shapes = tuple(jax.ShapeDtypeStruct(s, d) for s, d in outs)
    return pl.pallas_call(
        kernel,
        out_shape=shapes,
        in_specs=specs,
        out_specs=tuple(pl.BlockSpec(memory_space=pltpu.VMEM) for _ in shapes),
        scratch_shapes=list(scratch),
        cost_estimate=pl.CostEstimate(flops=flops, bytes_accessed=1 << 20, transcendentals=0),
        compiler_params=pltpu.CompilerParams(vmem_limit_bytes=VMEM_LIMIT),
    )(*args)


def traded(x, axes):
    return lax.all_to_all(x, axes, 0, 0, tiled=True)


def partner(x, axis):
    return lax.ppermute(x, axis, [(0, 1), (1, 0)])


def swapped(x):
    return jnp.swapaxes(x[0, 0], 0, 1)


US = 400_000_000
VMEM_LIMIT = 16 << 20


def step(cot, qt, kt, vt, qs, ks, vs, wt, ws, gt, gs):
    norm_weight = 1.0 / math.sqrt(16 * 64 * 128)
    norm_gate = 1.0 / math.sqrt(64 * 128)
    col = ((WIDTH, TOK), BF16)
    core = lax.axis_index("c").astype(jnp.int32).reshape(1)
    half = lax.axis_index("xl").astype(jnp.int32).reshape(1)
    exchanged = traded(cot[0], SEQ)
    other_cot = partner(cot, "c")
    cot_t = cot.reshape(TOK, MODEL)
    wt_t = wt.T
    ws_t = ws.T
    q2, k2, v2 = (x.reshape(TOK, WIDTH) for x in (qt, kt, vt))
    att_t, q_t, k_t, v_t = call(functools.partial(forward_kernel, True), [col] * 4, q2, k2, v2, flops=4 * US)
    other_att = partner(att_t, "c")
    (selected,) = call(select_kernel, [((WIDTH, 2 * TOK), BF16)], core, cot_t, other_cot.reshape(TOK, MODEL), gt, scalars=1, flops=2 * US)
    block = (288, WIDTH)
    keep, send = call(functools.partial(product_kernel, norm_weight), [(block, F32), (block, BF16)], half, att_t, other_att, selected, scalars=1, flops=2 * US)
    came = partner(send, "xl")
    (terms,) = call(join_kernel, [((8, 36, WIDTH), BF16)], keep, came, flops=US)
    arrived = traded(terms, "y")
    part = ((1, MODEL), F32)
    d_t, part_t = call(project_kernel, [col, part], cot_t, gt, wt_t, att_t, flops=2 * US)
    q_s, k_s, v_s = (swapped(x) for x in (qs, ks, vs))
    (att_s,) = call(functools.partial(forward_kernel, False), [col], q_s, k_s, v_s, flops=3 * US)
    d_s, part_s = call(project_kernel, [col, part], exchanged.reshape(TOK, MODEL), gs, ws_t, att_s, flops=2 * US)
    came_gate = partner(jnp.where(core == 0, part_s, part_t), "c")
    (packed,) = call(pack_kernel, [((32, 16, 128), BF16)], core, arrived, part_t, part_s, came_gate, scalars=1, flops=US)
    rows = traded(packed, ROWS)
    tok = ((TOK, WIDTH), BF16)
    grads_t = call(functools.partial(backward_kernel, True), [tok] * 3, q_t, k_t, v_t, att_t, d_t, scratch=[pltpu.VMEM((WIDTH, TOK), F32)] * 3, flops=4 * US)
    grads_s = call(functools.partial(backward_kernel, False), [col] * 3, q_s, k_s, v_s, att_s, d_s, flops=4 * US)
    weight_grad, gate = call(functools.partial(finish_kernel, norm_gate), [((18, 36), F32), part], rows, flops=US)
    other_gate = partner(gate, "c")
    return (
        *(g.reshape(1, 64, 2, WIDTH) for g in grads_t),
        *(jnp.swapaxes(g, 0, 1)[None, None] for g in grads_s),
        weight_grad,
        jnp.where(core == 0, gate, other_gate),
        jnp.where(core == 0, other_gate, gate),
    )


def solution(mesh):
    fine = Mesh(np.array(mesh.devices).reshape(2, 8, 16, 2, 2), ("xl", "y", "z", "xh", "c"))
    by_pos = P(DP, None, SEQ, None)
    by_frame = P(DP, SEQ, None, None)
    in_specs = (by_pos,) * 4 + (by_frame,) * 3 + (P(), P(), P(DP, None), P(DP, None))
    out_specs = (by_pos,) * 3 + (by_frame,) * 3 + (P(SEQ, DP), P(DP, None), P(DP, None))
    return jax.shard_map(step, mesh=fine, in_specs=in_specs, out_specs=out_specs, check_vma=False)
```

```python
import functools
import math

import jax
import jax.numpy as jnp
import numpy as np
from jax import lax
from jax.experimental import pallas as pl
from jax.experimental.pallas import tpu as pltpu
from jax.sharding import Mesh
from jax.sharding import PartitionSpec as P

HD = 72
HEADS = 8
WIDTH = 576
MODEL = 1152
TOK = 128
NT = (((1,), (1,)), ((), ()))
TN = (((0,), (0,)), ((), ()))
NN = (((1,), (0,)), ((), ()))
F32 = jnp.float32
BF16 = jnp.bfloat16
DP = ("xl", "y")
SEQ = ("z", "xh", "c")
ROWS = ("z", "xh")
SCALE = 1.0 / math.sqrt(HD)


def dot(a, b, dims):
    return lax.dot_general(a, b, dims, preferred_element_type=F32)


def probs_of(key, query, keep):
    scores = dot(key, query, TN) * SCALE
    if keep is not None:
        scores = jnp.where(keep, scores, -jnp.inf)
    top = jnp.max(scores, axis=0, keepdims=True)
    e = jnp.exp(scores - top)
    return e / jnp.sum(e, axis=0, keepdims=True)


def same_position():
    i = lax.broadcasted_iota(jnp.int32, (TOK, TOK), 0)
    j = lax.broadcasted_iota(jnp.int32, (TOK, TOK), 1)
    return ((i + j) & 1) == 0


def turned(x):
    return x.astype(F32).T.astype(BF16)


def rows_of(ref, h):
    return ref[h * HD : (h + 1) * HD, :]


def forward_kernel(q_ref, k_ref, v_ref, out_ref):
    for h in range(HEADS):
        low = probs_of(rows_of(k_ref, h), rows_of(q_ref, h), None).astype(BF16)
        out_ref[h * HD : (h + 1) * HD, :] = dot(rows_of(v_ref, h), low, NN).astype(BF16)


def flat(ref):
    x = ref[...]
    return x.reshape(TOK, x.shape[-1])


def picked(core, gated):
    row = lax.broadcasted_iota(jnp.int32, (WIDTH, 1), 0)
    block = (row * 3641) >> 16
    channel = row + 18 * (block + core)
    col = lax.broadcasted_iota(jnp.int32, (WIDTH, MODEL), 1)
    pick = jnp.where(col == channel, 1.0, 0.0).astype(BF16)
    return dot(pick, gated, NT).astype(BF16)


def start_kernel(core_ref, gate_ref, *rest):
    sources, (send_ref, own_ref), landed, (q_t, k_t, v_t, sems) = rest[:4], rest[4:6], rest[6:10], rest[10:]
    copies = [pltpu.make_async_copy(a, b, sems.at[i]) for i, (a, b) in enumerate(zip(sources, landed))]
    for copy in copies:
        copy.start()
    keep = same_position()
    for copy in copies:
        copy.wait()
    q_ref, k_ref, v_ref, cot_ref = landed
    for src, dst in zip((q_ref, k_ref, v_ref), (q_t, k_t, v_t)):
        dst[...] = turned(flat(src))
    for h in range(HEADS):
        low = probs_of(rows_of(k_t, h), rows_of(q_t, h), keep).astype(BF16)
        send_ref[h * HD : (h + 1) * HD, :] = dot(rows_of(v_t, h), low, NN).astype(BF16)
    gated = (flat(cot_ref).astype(F32) * gate_ref[...]).astype(BF16)
    core = core_ref[0]
    own_ref[...] = picked(core, gated)
    send_ref[WIDTH:, :] = picked(1 - core, gated)


def project_kernel(cot_ref, gate_ref, w_ref, att_ref, d_ref, part_ref):
    cot = flat(cot_ref).astype(F32)
    gated = (cot * gate_ref[...]).astype(BF16)
    d_ref[...] = dot(w_ref[...], gated, NT).astype(BF16)
    projected = dot(att_ref[:WIDTH, :], w_ref[...], TN)
    part_ref[...] = jnp.sum(cot * projected, axis=0, keepdims=True)


def backward_kernel(over_time, q_ref, k_ref, v_ref, att_ref, d_ref, gq_ref, gk_ref, gv_ref, *scratch):
    keep = same_position() if over_time else None
    outs = (gq_ref, gk_ref, gv_ref)
    if over_time:
        for src, dst in zip((q_ref, k_ref, v_ref), scratch):
            dst[...] = turned(flat(src))
        q_ref, k_ref, v_ref = scratch[:3]
        outs = scratch[3:]
    for h in range(HEADS):
        sl = slice(h * HD, (h + 1) * HD)
        q, k, v, a, d = (rows_of(r, h) for r in (q_ref, k_ref, v_ref, att_ref, d_ref))
        probs = probs_of(k, q, keep)
        low = probs.astype(BF16)
        d_probs = dot(v, d, TN)
        delta = jnp.sum(d.astype(F32) * a.astype(F32), axis=0, keepdims=True)
        d_scores = (probs * (d_probs - delta)).astype(BF16)
        grads = (dot(k, d_scores, NN) * SCALE, dot(q, d_scores, NT) * SCALE, dot(d, low, NT))
        for ref, g in zip(outs, grads):
            ref[sl, :] = g.astype(ref.dtype)
    if over_time:
        for src, dst in zip(outs, (gq_ref, gk_ref, gv_ref)):
            dst[...] = src[...].T.astype(BF16).reshape(dst.shape)


def product_kernel(norm, y_ref, mine_ref, own_ref, came_ref, keep_ref, *rest):
    sends, total = rest[:7], rest[7]
    terms = dot(mine_ref[:WIDTH, :], own_ref[...], NT) + dot(came_ref[:WIDTH, :], came_ref[WIDTH:, :], NT)
    terms = terms * norm
    for i in range(16):
        total[40 * i : 40 * i + 36, :] = terms[36 * i : 36 * i + 36, :]
    y = y_ref[0]

    def block(at):
        at = jnp.where(at >= 8, at - 8, at)
        parts = [total[pl.ds(pl.multiple_of(320 * x + 40 * at, 8), 40), :][:36] for x in (0, 1)]
        return jnp.concatenate(parts, axis=0)

    keep_ref[...] = block(y)
    for shift, ref in enumerate(sends, 1):
        ref[...] = block(y + shift).astype(BF16)


def gather_kernel(half_ref, keep_ref, *rest):
    came, (own_ref, send_ref) = rest[:7], rest[7:]
    total = keep_ref[...]
    for ref in came:
        total = total + ref[...].astype(F32)
    first = half_ref[0] == 0
    low, high = total[:36], total[36:]
    own_ref[...] = jnp.where(first, low, high)
    send_ref[...] = jnp.where(first, high, low).astype(BF16)


def pack_kernel(core_ref, own_ref, in_ref, time_ref, space_ref, came_ref, out_ref):
    total = own_ref[...] + in_ref[...].astype(F32)
    total = jnp.concatenate([total, jnp.zeros((4, WIDTH), F32)], axis=0)
    gate = jnp.where(core_ref[0] == 0, time_ref[...], space_ref[...]) + came_ref[...]
    last = gate[:, 1024:]
    tail = jnp.concatenate([last[:, 16 * a : 16 * a + 16] for a in range(8)], axis=0)
    gap = jnp.zeros((8, 22), F32)
    low = jnp.concatenate([gate[:, 128 * a : 128 * a + 128] for a in range(8)], axis=0)
    for m in range(32):
        parts = [total[8 * b : 8 * b + 8, 18 * m : 18 * m + 18] for b in range(5)]
        high = jnp.concatenate(parts + [gap, tail], axis=1)
        out_ref[m] = jnp.concatenate([high, low], axis=0).astype(BF16)


def finish_kernel(norm, in_ref, out_ref, gate_ref):
    total = jnp.sum(in_ref[...].astype(F32), axis=0)
    high = total[:8]
    flipped = high.T
    for b in range(5):
        n = 8 if b < 4 else 4
        out_ref[:, 8 * b : 8 * b + n] = flipped[18 * b : 18 * b + 18, :n]
    for a in range(8):
        gate_ref[:, 128 * a : 128 * a + 128] = total[8 + a : 9 + a, :] * norm
    last = jnp.concatenate([high[a : a + 1, 112:] for a in range(8)], axis=1)
    gate_ref[:, 1024:] = last * norm


US = 400_000_000
VMEM_LIMIT = 16 << 20
FULL = 66_000_000


def call(kernel, outs, *args, scratch=(), flops=0, scalars=0, far=0, vmem=VMEM_LIMIT):
    specs = [pl.BlockSpec(memory_space=pltpu.SMEM)] * scalars
    specs += [pl.BlockSpec(memory_space=pltpu.VMEM)] * (len(args) - scalars - far)
    specs += [pl.BlockSpec(memory_space=pltpu.HBM)] * far
    shapes = tuple(jax.ShapeDtypeStruct(s, d) for s, d in outs)
    return pl.pallas_call(
        kernel,
        out_shape=shapes,
        in_specs=specs,
        out_specs=tuple(pl.BlockSpec(memory_space=pltpu.VMEM) for _ in shapes),
        scratch_shapes=list(scratch),
        cost_estimate=pl.CostEstimate(flops=flops, bytes_accessed=1 << 20, transcendentals=0),
        compiler_params=pltpu.CompilerParams(vmem_limit_bytes=vmem),
    )(*args)


def traded(x, axes):
    return lax.all_to_all(x, axes, 0, 0, tiled=True)


def partner(x, axis):
    return lax.ppermute(x, axis, [(0, 1), (1, 0)])


def shifted(x, axis, step, size):
    return lax.ppermute(x, axis, [(i, (i + step) % size) for i in range(size)])


def swapped(x):
    return jnp.swapaxes(x[0, 0], 0, 1)


def step(cot, qt, kt, vt, qs, ks, vs, wt, ws, gt, gs):
    norm_weight = 1.0 / math.sqrt(16 * 64 * 128)
    norm_gate = 1.0 / math.sqrt(64 * 128)
    col = ((WIDTH, TOK), BF16)
    core = lax.axis_index("c").astype(jnp.int32).reshape(1)
    half = lax.axis_index("xl").astype(jnp.int32).reshape(1)
    place = lax.axis_index("y").astype(jnp.int32).reshape(1)
    exchanged = traded(cot[0], SEQ)
    cot_t = cot[0]
    wt_t = wt.T
    ws_t = ws.T
    time_in = (qt[0], kt[0], vt[0])
    turned_in = [pltpu.VMEM((WIDTH, TOK), BF16)] * 3
    landing = [pltpu.VMEM(x.shape, BF16) for x in (*time_in, cot_t)]
    mine, own_rows = call(start_kernel, [((2 * WIDTH, TOK), BF16), col], core, gt, *time_in, cot_t, scratch=landing + turned_in + [pltpu.SemaphoreType.DMA((4,))], scalars=1, far=4, vmem=FULL, flops=4 * US)
    came = partner(mine, "c")
    block = (72, WIDTH)
    keep, *sends = call(functools.partial(product_kernel, norm_weight), [(block, F32)] + [(block, BF16)] * 7, place, mine, own_rows, came, scratch=[pltpu.VMEM((640, WIDTH), F32)], scalars=1, flops=2 * US)
    blocks = [shifted(x, "y", k, 8) for k, x in enumerate(sends, 1)]
    part_rows = (36, WIDTH)
    own_half, send_half = call(gather_kernel, [(part_rows, F32), (part_rows, BF16)], half, keep, *blocks, scalars=1, flops=US)
    came_half = partner(send_half, "xl")
    part = ((1, MODEL), F32)
    d_t, part_t = call(project_kernel, [col, part], cot_t, gt, wt_t, mine, flops=2 * US)
    q_s, k_s, v_s = (swapped(x) for x in (qs, ks, vs))
    (att_s,) = call(forward_kernel, [col], q_s, k_s, v_s, flops=3 * US)
    d_s, part_s = call(project_kernel, [col, part], exchanged, gs, ws_t, att_s, flops=2 * US)
    came_gate = partner(jnp.where(core == 0, part_s, part_t), "c")
    (packed,) = call(pack_kernel, [((32, 16, 128), BF16)], core, own_half, came_half, part_t, part_s, came_gate, scalars=1, flops=US)
    rows = traded(packed, ROWS)
    tok = ((64, 2, WIDTH), BF16)
    grads_t = call(functools.partial(backward_kernel, True), [tok] * 3, *time_in, mine, d_t, scratch=turned_in + [pltpu.VMEM((WIDTH, TOK), F32)] * 3, flops=4 * US)
    grads_s = call(functools.partial(backward_kernel, False), [col] * 3, q_s, k_s, v_s, att_s, d_s, flops=4 * US)
    weight_grad, gate = call(functools.partial(finish_kernel, norm_gate), [((18, 36), F32), part], rows, flops=US)
    other_gate = partner(gate, "c")
    return (
        *(g[None] for g in grads_t),
        *(jnp.swapaxes(g, 0, 1)[None, None] for g in grads_s),
        weight_grad,
        jnp.where(core == 0, gate, other_gate),
        jnp.where(core == 0, other_gate, gate),
    )


def solution(mesh):
    fine = Mesh(np.array(mesh.devices).reshape(2, 8, 16, 2, 2), ("xl", "y", "z", "xh", "c"))
    by_pos = P(DP, None, SEQ, None)
    by_frame = P(DP, SEQ, None, None)
    in_specs = (by_pos,) * 4 + (by_frame,) * 3 + (P(), P(), P(DP, None), P(DP, None))
    out_specs = (by_pos,) * 3 + (by_frame,) * 3 + (P(SEQ, DP), P(DP, None), P(DP, None))
    return jax.shard_map(step, mesh=fine, in_specs=in_specs, out_specs=out_specs, check_vma=False)
```

```python
import functools
import math

import jax
import jax.numpy as jnp
import numpy as np
from jax import lax
from jax.experimental import pallas as pl
from jax.experimental.pallas import tpu as pltpu
from jax.sharding import Mesh
from jax.sharding import PartitionSpec as P

HD = 72
HEADS = 8
WIDTH = 576
MODEL = 1152
TOK = 128
NT = (((1,), (1,)), ((), ()))
TN = (((0,), (0,)), ((), ()))
NN = (((1,), (0,)), ((), ()))
F32 = jnp.float32
BF16 = jnp.bfloat16
DP = ("xl", "y")
SEQ = ("z", "xh", "c")
ROWS = ("z", "xh")
SCALE = 1.0 / math.sqrt(HD)


def dot(a, b, dims):
    return lax.dot_general(a, b, dims, preferred_element_type=F32)


def probs_of(key, query, keep):
    scores = dot(key, query, TN) * SCALE
    if keep is not None:
        scores = jnp.where(keep, scores, -jnp.inf)
    top = jnp.max(scores, axis=0, keepdims=True)
    e = jnp.exp(scores - top)
    return e / jnp.sum(e, axis=0, keepdims=True)


def same_position():
    i = lax.broadcasted_iota(jnp.int32, (TOK, TOK), 0)
    j = lax.broadcasted_iota(jnp.int32, (TOK, TOK), 1)
    return ((i + j) & 1) == 0


def turned(x):
    return x.astype(F32).T.astype(BF16)


def rows_of(ref, h):
    return ref[h * HD : (h + 1) * HD, :]


def flat(ref):
    x = ref[...]
    return x.reshape(TOK, x.shape[-1])


def forward_kernel(over_time, q_ref, k_ref, v_ref, out_ref, *turned_refs):
    keep = same_position() if over_time else None
    if over_time:
        for src, dst in zip((q_ref, k_ref, v_ref), turned_refs):
            dst[...] = turned(src[...])
        q_ref, k_ref, v_ref = turned_refs
    for h in range(HEADS):
        low = probs_of(rows_of(k_ref, h), rows_of(q_ref, h), keep).astype(BF16)
        out_ref[h * HD : (h + 1) * HD, :] = dot(rows_of(v_ref, h), low, NN).astype(BF16)


def project_kernel(cot_ref, gate_ref, w_ref, att_ref, d_ref, part_ref):
    cot = flat(cot_ref).astype(F32)
    gated = (cot * gate_ref[...]).astype(BF16)
    d_ref[...] = dot(w_ref[...], gated, NT).astype(BF16)
    projected = dot(att_ref[...], w_ref[...], TN)
    part_ref[...] = jnp.sum(cot * projected, axis=0, keepdims=True)


def backward_kernel(over_time, q_ref, k_ref, v_ref, att_ref, d_ref, gq_ref, gk_ref, gv_ref, *scratch):
    keep = same_position() if over_time else None
    outs = (gq_ref, gk_ref, gv_ref)
    if over_time:
        for src, dst in zip((q_ref, k_ref, v_ref), scratch):
            dst[...] = turned(flat(src))
        q_ref, k_ref, v_ref = scratch[:3]
        outs = scratch[3:]
    for h in range(HEADS):
        sl = slice(h * HD, (h + 1) * HD)
        q, k, v, a, d = (rows_of(r, h) for r in (q_ref, k_ref, v_ref, att_ref, d_ref))
        probs = probs_of(k, q, keep)
        low = probs.astype(BF16)
        d_probs = dot(v, d, TN)
        delta = jnp.sum(d.astype(F32) * a.astype(F32), axis=0, keepdims=True)
        d_scores = (probs * (d_probs - delta)).astype(BF16)
        grads = (dot(k, d_scores, NN) * SCALE, dot(q, d_scores, NT) * SCALE, dot(d, low, NT))
        for ref, g in zip(outs, grads):
            ref[sl, :] = g.astype(ref.dtype)
    if over_time:
        for src, dst in zip(outs, (gq_ref, gk_ref, gv_ref)):
            dst[...] = src[...].T.astype(BF16).reshape(dst.shape)


def select_kernel(core_ref, own_ref, other_ref, gate_ref, out_ref):
    core = core_ref[0]
    row = lax.broadcasted_iota(jnp.int32, (WIDTH, 1), 0)
    block = (row * 3641) >> 16
    channel = row + 18 * (block + core)
    col = lax.broadcasted_iota(jnp.int32, (WIDTH, MODEL), 1)
    pick = jnp.where(col == channel, 1.0, 0.0).astype(BF16)
    for i, ref in enumerate((own_ref, other_ref)):
        gated = (flat(ref).astype(F32) * gate_ref[...]).astype(BF16)
        out_ref[:, i * TOK : (i + 1) * TOK] = dot(pick, gated, NT).astype(BF16)


def product_kernel(norm, half_ref, own_ref, other_ref, sel_ref, keep_ref, send_ref):
    half = half_ref[0]
    sel = sel_ref[...]
    for ref, index in ((keep_ref, half), (send_ref, 1 - half)):
        rows = pl.ds(pl.multiple_of(index * 288, 32), 288)
        att = jnp.concatenate([own_ref[rows, :], other_ref[rows, :]], axis=1)
        term = dot(att, sel, NT) * norm
        for y in range(8):
            block = term[36 * y : 36 * y + 36]
            tiles = [block[:, 128 * t : 128 * t + 128] for t in range(4)]
            last = jnp.concatenate([block[:18, 512:], block[18:, 512:]], axis=1)
            ref[y] = jnp.concatenate(tiles + [last], axis=0).astype(ref.dtype)


def join_kernel(keep_ref, came_ref, out_ref):
    out_ref[...] = (keep_ref[...] + came_ref[...].astype(F32)).astype(BF16)


def pack_kernel(core_ref, in_ref, time_ref, space_ref, came_ref, out_ref):
    total = jnp.sum(in_ref[...].astype(F32), axis=0)
    last = jnp.concatenate([total[144:, :64], total[144:, 64:]], axis=0)
    tiles = [total[36 * t : 36 * t + 36] for t in range(4)]
    total = jnp.concatenate(tiles + [last], axis=1)
    total = jnp.concatenate([total, jnp.zeros((4, WIDTH), F32)], axis=0)
    gate = jnp.where(core_ref[0] == 0, time_ref[...], space_ref[...]) + came_ref[...]
    last = gate[:, 1024:]
    tail = jnp.concatenate([last[:, 16 * a : 16 * a + 16] for a in range(8)], axis=0)
    gap = jnp.zeros((8, 22), F32)
    low = jnp.concatenate([gate[:, 128 * a : 128 * a + 128] for a in range(8)], axis=0)
    for m in range(32):
        parts = [total[8 * b : 8 * b + 8, 18 * m : 18 * m + 18] for b in range(5)]
        high = jnp.concatenate(parts + [gap, tail], axis=1)
        out_ref[m] = jnp.concatenate([high, low], axis=0).astype(BF16)


def finish_kernel(norm, in_ref, out_ref, gate_ref):
    total = jnp.sum(in_ref[...].astype(F32), axis=0)
    high = total[:8]
    flipped = high.T
    for b in range(5):
        n = 8 if b < 4 else 4
        out_ref[:, 8 * b : 8 * b + n] = flipped[18 * b : 18 * b + 18, :n]
    for a in range(8):
        gate_ref[:, 128 * a : 128 * a + 128] = total[8 + a : 9 + a, :] * norm
    last = jnp.concatenate([high[a : a + 1, 112:] for a in range(8)], axis=1)
    gate_ref[:, 1024:] = last * norm


def call(kernel, outs, *args, scratch=(), flops=0, scalars=0):
    specs = [pl.BlockSpec(memory_space=pltpu.SMEM)] * scalars
    specs += [pl.BlockSpec(memory_space=pltpu.VMEM)] * (len(args) - scalars)
    shapes = tuple(jax.ShapeDtypeStruct(s, d) for s, d in outs)
    return pl.pallas_call(
        kernel,
        out_shape=shapes,
        in_specs=specs,
        out_specs=tuple(pl.BlockSpec(memory_space=pltpu.VMEM) for _ in shapes),
        scratch_shapes=list(scratch),
        cost_estimate=pl.CostEstimate(flops=flops, bytes_accessed=1 << 20, transcendentals=0),
        compiler_params=pltpu.CompilerParams(vmem_limit_bytes=VMEM_LIMIT),
    )(*args)


def traded(x, axes):
    return lax.all_to_all(x, axes, 0, 0, tiled=True)


def partner(x, axis):
    return lax.ppermute(x, axis, [(0, 1), (1, 0)])


def swapped(x):
    return jnp.swapaxes(x[0, 0], 0, 1)


US = 400_000_000
VMEM_LIMIT = 16 << 20


def step(cot, qt, kt, vt, qs, ks, vs, wt, ws, gt, gs):
    norm_weight = 1.0 / math.sqrt(16 * 64 * 128)
    norm_gate = 1.0 / math.sqrt(64 * 128)
    col = ((WIDTH, TOK), BF16)
    core = lax.axis_index("c").astype(jnp.int32).reshape(1)
    half = lax.axis_index("xl").astype(jnp.int32).reshape(1)
    exchanged = traded(cot[0], SEQ)
    other_cot = partner(cot, "c")
    cot_t = cot[0]
    wt_t = wt.T
    ws_t = ws.T
    turned_in = [pltpu.VMEM((WIDTH, TOK), BF16)] * 3
    q2, k2, v2 = (x.reshape(TOK, WIDTH) for x in (qt, kt, vt))
    (att_t,) = call(functools.partial(forward_kernel, True), [col], q2, k2, v2, scratch=turned_in, flops=4 * US)
    other_att = partner(att_t, "c")
    (selected,) = call(select_kernel, [((WIDTH, 2 * TOK), BF16)], core, cot_t, other_cot[0], gt, scalars=1, flops=2 * US)
    block = (8, 162, 128)
    keep, send = call(functools.partial(product_kernel, norm_weight), [(block, F32), (block, BF16)], half, att_t, other_att, selected, scalars=1, flops=2 * US)
    came = partner(send, "xl")
    (terms,) = call(join_kernel, [(block, BF16)], keep, came, flops=US)
    arrived = traded(terms, "y")
    part = ((1, MODEL), F32)
    d_t, part_t = call(project_kernel, [col, part], cot_t, gt, wt_t, att_t, flops=2 * US)
    q_s, k_s, v_s = (swapped(x) for x in (qs, ks, vs))
    (att_s,) = call(functools.partial(forward_kernel, False), [col], q_s, k_s, v_s, flops=3 * US)
    d_s, part_s = call(project_kernel, [col, part], exchanged, gs, ws_t, att_s, flops=2 * US)
    came_gate = partner(jnp.where(core == 0, part_s, part_t), "c")
    (packed,) = call(pack_kernel, [((32, 16, 128), BF16)], core, arrived, part_t, part_s, came_gate, scalars=1, flops=US)
    rows = traded(packed, ROWS)
    tok = ((64, 2, WIDTH), BF16)
    grads_t = call(functools.partial(backward_kernel, True), [tok] * 3, qt[0], kt[0], vt[0], att_t, d_t, scratch=turned_in + [pltpu.VMEM((WIDTH, TOK), F32)] * 3, flops=4 * US)
    grads_s = call(functools.partial(backward_kernel, False), [col] * 3, q_s, k_s, v_s, att_s, d_s, flops=4 * US)
    weight_grad, gate = call(functools.partial(finish_kernel, norm_gate), [((18, 36), F32), part], rows, flops=US)
    other_gate = partner(gate, "c")
    return (
        *(g[None] for g in grads_t),
        *(jnp.swapaxes(g, 0, 1)[None, None] for g in grads_s),
        weight_grad,
        jnp.where(core == 0, gate, other_gate),
        jnp.where(core == 0, other_gate, gate),
    )


def solution(mesh):
    fine = Mesh(np.array(mesh.devices).reshape(2, 8, 16, 2, 2), ("xl", "y", "z", "xh", "c"))
    by_pos = P(DP, None, SEQ, None)
    by_frame = P(DP, SEQ, None, None)
    in_specs = (by_pos,) * 4 + (by_frame,) * 3 + (P(), P(), P(DP, None), P(DP, None))
    out_specs = (by_pos,) * 3 + (by_frame,) * 3 + (P(SEQ, DP), P(DP, None), P(DP, None))
    return jax.shard_map(step, mesh=fine, in_specs=in_specs, out_specs=out_specs, check_vma=False)
```

```python
import functools
import math

import jax
import jax.numpy as jnp
import numpy as np
from jax import lax
from jax.experimental import pallas as pl
from jax.experimental.pallas import tpu as pltpu
from jax.sharding import Mesh
from jax.sharding import PartitionSpec as P

HD = 72
HEADS = 8
WIDTH = 576
MODEL = 1152
TOK = 128
NT = (((1,), (1,)), ((), ()))
TN = (((0,), (0,)), ((), ()))
NN = (((1,), (0,)), ((), ()))
F32 = jnp.float32
BF16 = jnp.bfloat16
DP = ("xl", "yh", "yl")
PAIRS = ("xl", "yh")
SEQ = ("z", "xh", "c")
ROWS = ("z", "xh")
SCALE = 1.0 / math.sqrt(HD)


def dot(a, b, dims):
    return lax.dot_general(a, b, dims, preferred_element_type=F32)


def probs_of(key, query, keep):
    scores = dot(key, query, TN) * SCALE
    if keep is not None:
        scores = jnp.where(keep, scores, -jnp.inf)
    top = jnp.max(scores, axis=0, keepdims=True)
    e = jnp.exp(scores - top)
    return e / jnp.sum(e, axis=0, keepdims=True)


def same_position():
    i = lax.broadcasted_iota(jnp.int32, (TOK, TOK), 0)
    j = lax.broadcasted_iota(jnp.int32, (TOK, TOK), 1)
    return ((i + j) & 1) == 0


def turned(x):
    return x.astype(F32).T.astype(BF16)


def rows_of(ref, h):
    return ref[h * HD : (h + 1) * HD, :]


def flat(ref):
    x = ref[...]
    return x.reshape(TOK, x.shape[-1])


def forward_kernel(over_time, q_ref, k_ref, v_ref, out_ref, *turned_refs):
    keep = same_position() if over_time else None
    if over_time:
        for src, dst in zip((q_ref, k_ref, v_ref), turned_refs):
            dst[...] = turned(src[...])
        q_ref, k_ref, v_ref = turned_refs
    for h in range(HEADS):
        low = probs_of(rows_of(k_ref, h), rows_of(q_ref, h), keep).astype(BF16)
        out_ref[h * HD : (h + 1) * HD, :] = dot(rows_of(v_ref, h), low, NN).astype(BF16)


def project_kernel(cot_ref, gate_ref, w_ref, att_ref, d_ref, part_ref):
    cot = flat(cot_ref).astype(F32)
    gated = (cot * gate_ref[...]).astype(BF16)
    d_ref[...] = dot(w_ref[...], gated, NT).astype(BF16)
    projected = dot(att_ref[...], w_ref[...], TN)
    part_ref[...] = jnp.sum(cot * projected, axis=0, keepdims=True)


def backward_kernel(over_time, q_ref, k_ref, v_ref, att_ref, d_ref, gq_ref, gk_ref, gv_ref, *scratch):
    keep = same_position() if over_time else None
    outs = (gq_ref, gk_ref, gv_ref)
    if over_time:
        for src, dst in zip((q_ref, k_ref, v_ref), scratch):
            dst[...] = turned(flat(src))
        q_ref, k_ref, v_ref = scratch[:3]
        outs = scratch[3:]
    for h in range(HEADS):
        sl = slice(h * HD, (h + 1) * HD)
        q, k, v, a, d = (rows_of(r, h) for r in (q_ref, k_ref, v_ref, att_ref, d_ref))
        probs = probs_of(k, q, keep)
        low = probs.astype(BF16)
        d_probs = dot(v, d, TN)
        delta = jnp.sum(d.astype(F32) * a.astype(F32), axis=0, keepdims=True)
        d_scores = (probs * (d_probs - delta)).astype(BF16)
        grads = (dot(k, d_scores, NN) * SCALE, dot(q, d_scores, NT) * SCALE, dot(d, low, NT))
        for ref, g in zip(outs, grads):
            ref[sl, :] = g.astype(ref.dtype)
    if over_time:
        for src, dst in zip(outs, (gq_ref, gk_ref, gv_ref)):
            dst[...] = src[...].T.astype(BF16).reshape(dst.shape)


def select_kernel(core_ref, own_ref, other_ref, gate_ref, out_ref):
    core = core_ref[0]
    row = lax.broadcasted_iota(jnp.int32, (WIDTH, 1), 0)
    block = (row * 3641) >> 16
    channel = row + 18 * (block + core)
    col = lax.broadcasted_iota(jnp.int32, (WIDTH, MODEL), 1)
    pick = jnp.where(col == channel, 1.0, 0.0).astype(BF16)
    for i, ref in enumerate((own_ref, other_ref)):
        gated = (flat(ref).astype(F32) * gate_ref[...]).astype(BF16)
        out_ref[:, i * TOK : (i + 1) * TOK] = dot(pick, gated, NT).astype(BF16)


def packed_block(block):
    tiles = [block[:, 128 * t : 128 * t + 128] for t in range(4)]
    last = jnp.concatenate([block[:18, 512:], block[18:, 512:]], axis=1)
    return jnp.concatenate(tiles + [last], axis=0)


def product_kernel(norm, half_ref, own_ref, other_ref, sel_ref, keep_ref, send_ref):
    first = half_ref[0] == 0
    att = jnp.concatenate([own_ref[...], other_ref[...]], axis=1)
    term = dot(att, sel_ref[...], NT) * norm
    for g in range(8):
        low = packed_block(term[HD * g : HD * g + 36])
        high = packed_block(term[HD * g + 36 : HD * g + HD])
        keep_ref[g] = jnp.where(first, low, high)
        send_ref[g] = jnp.where(first, high, low).astype(BF16)


def join_kernel(keep_ref, came_ref, out_ref):
    out_ref[...] = (keep_ref[...] + came_ref[...].astype(F32)).astype(BF16)


def pack_kernel(core_ref, in_ref, time_ref, space_ref, came_ref, out_ref):
    total = jnp.sum(in_ref[...].astype(F32), axis=0)
    last = jnp.concatenate([total[144:, :64], total[144:, 64:]], axis=0)
    tiles = [total[36 * t : 36 * t + 36] for t in range(4)]
    total = jnp.concatenate(tiles + [last], axis=1)
    total = jnp.concatenate([total, jnp.zeros((4, WIDTH), F32)], axis=0)
    gate = jnp.where(core_ref[0] == 0, time_ref[...], space_ref[...]) + came_ref[...]
    last = gate[:, 1024:]
    tail = jnp.concatenate([last[:, 16 * a : 16 * a + 16] for a in range(8)], axis=0)
    gap = jnp.zeros((8, 22), F32)
    low = jnp.concatenate([gate[:, 128 * a : 128 * a + 128] for a in range(8)], axis=0)
    for m in range(32):
        parts = [total[8 * b : 8 * b + 8, 18 * m : 18 * m + 18] for b in range(5)]
        high = jnp.concatenate(parts + [gap, tail], axis=1)
        out_ref[m] = jnp.concatenate([high, low], axis=0).astype(BF16)


def finish_kernel(norm, in_ref, out_ref, gate_ref):
    total = jnp.sum(in_ref[...].astype(F32), axis=0)
    high = total[:8]
    flipped = high.T
    for b in range(5):
        n = 8 if b < 4 else 4
        out_ref[:, 8 * b : 8 * b + n] = flipped[18 * b : 18 * b + 18, :n]
    for a in range(8):
        gate_ref[:, 128 * a : 128 * a + 128] = total[8 + a : 9 + a, :] * norm
    last = jnp.concatenate([high[a : a + 1, 112:] for a in range(8)], axis=1)
    gate_ref[:, 1024:] = last * norm


def call(kernel, outs, *args, scratch=(), flops=0, scalars=0):
    specs = [pl.BlockSpec(memory_space=pltpu.SMEM)] * scalars
    specs += [pl.BlockSpec(memory_space=pltpu.VMEM)] * (len(args) - scalars)
    shapes = tuple(jax.ShapeDtypeStruct(s, d) for s, d in outs)
    return pl.pallas_call(
        kernel,
        out_shape=shapes,
        in_specs=specs,
        out_specs=tuple(pl.BlockSpec(memory_space=pltpu.VMEM) for _ in shapes),
        scratch_shapes=list(scratch),
        cost_estimate=pl.CostEstimate(flops=flops, bytes_accessed=1 << 20, transcendentals=0),
        compiler_params=pltpu.CompilerParams(vmem_limit_bytes=VMEM_LIMIT),
    )(*args)


def traded(x, axes):
    return lax.all_to_all(x, axes, 0, 0, tiled=True)


def partner(x, axis):
    return lax.ppermute(x, axis, [(0, 1), (1, 0)])


def swapped(x):
    return jnp.swapaxes(x[0, 0], 0, 1)


US = 400_000_000
VMEM_LIMIT = 16 << 20


def step(cot, qt, kt, vt, qs, ks, vs, wt, ws, gt, gs):
    norm_weight = 1.0 / math.sqrt(16 * 64 * 128)
    norm_gate = 1.0 / math.sqrt(64 * 128)
    col = ((WIDTH, TOK), BF16)
    core = lax.axis_index("c").astype(jnp.int32).reshape(1)
    half = lax.axis_index("yl").astype(jnp.int32).reshape(1)
    exchanged = traded(cot[0], SEQ)
    other_cot = partner(cot, "c")
    cot_t = cot[0]
    wt_t = wt.T
    ws_t = ws.T
    turned_in = [pltpu.VMEM((WIDTH, TOK), BF16)] * 3
    q2, k2, v2 = (x.reshape(TOK, WIDTH) for x in (qt, kt, vt))
    (att_t,) = call(functools.partial(forward_kernel, True), [col], q2, k2, v2, scratch=turned_in, flops=4 * US)
    other_att = partner(att_t, "c")
    (selected,) = call(select_kernel, [((WIDTH, 2 * TOK), BF16)], core, cot_t, other_cot[0], gt, scalars=1, flops=2 * US)
    block = (8, 162, 128)
    keep, send = call(functools.partial(product_kernel, norm_weight), [(block, F32), (block, BF16)], half, att_t, other_att, selected, scalars=1, flops=2 * US)
    came = partner(send, "yl")
    (terms,) = call(join_kernel, [(block, BF16)], keep, came, flops=US)
    arrived = traded(terms, PAIRS)
    part = ((1, MODEL), F32)
    d_t, part_t = call(project_kernel, [col, part], cot_t, gt, wt_t, att_t, flops=2 * US)
    q_s, k_s, v_s = (swapped(x) for x in (qs, ks, vs))
    (att_s,) = call(functools.partial(forward_kernel, False), [col], q_s, k_s, v_s, flops=3 * US)
    d_s, part_s = call(project_kernel, [col, part], exchanged, gs, ws_t, att_s, flops=2 * US)
    came_gate = partner(jnp.where(core == 0, part_s, part_t), "c")
    (packed,) = call(pack_kernel, [((32, 16, 128), BF16)], core, arrived, part_t, part_s, came_gate, scalars=1, flops=US)
    rows = traded(packed, ROWS)
    tok = ((64, 2, WIDTH), BF16)
    grads_t = call(functools.partial(backward_kernel, True), [tok] * 3, qt[0], kt[0], vt[0], att_t, d_t, scratch=turned_in + [pltpu.VMEM((WIDTH, TOK), F32)] * 3, flops=4 * US)
    grads_s = call(functools.partial(backward_kernel, False), [col] * 3, q_s, k_s, v_s, att_s, d_s, flops=4 * US)
    weight_grad, gate = call(functools.partial(finish_kernel, norm_gate), [((18, 36), F32), part], rows, flops=US)
    other_gate = partner(gate, "c")
    return (
        *(g[None] for g in grads_t),
        *(jnp.swapaxes(g, 0, 1)[None, None] for g in grads_s),
        weight_grad,
        jnp.where(core == 0, gate, other_gate),
        jnp.where(core == 0, other_gate, gate),
    )


def solution(mesh):
    fine = Mesh(np.array(mesh.devices).reshape(2, 4, 2, 16, 2, 2), ("xl", "yh", "yl", "z", "xh", "c"))
    by_pos = P(DP, None, SEQ, None)
    by_frame = P(DP, SEQ, None, None)
    in_specs = (by_pos,) * 4 + (by_frame,) * 3 + (P(), P(), P(DP, None), P(DP, None))
    out_specs = (by_pos,) * 3 + (by_frame,) * 3 + (P(SEQ, DP), P(DP, None), P(DP, None))
    return jax.shard_map(step, mesh=fine, in_specs=in_specs, out_specs=out_specs, check_vma=False)
```

```python
import functools
import math

import jax
import jax.numpy as jnp
import numpy as np
from jax import lax
from jax.experimental import pallas as pl
from jax.experimental.pallas import tpu as pltpu
from jax.sharding import Mesh
from jax.sharding import PartitionSpec as P

HD = 72
HEADS = 8
WIDTH = 576
MODEL = 1152
TOK = 128
NT = (((1,), (1,)), ((), ()))
TN = (((0,), (0,)), ((), ()))
NN = (((1,), (0,)), ((), ()))
F32 = jnp.float32
BF16 = jnp.bfloat16
DP = ("xl", "yh", "yl")
SEQ = ("z", "xh", "c")
ROWS = ("z", "xh")
SCALE = 1.0 / math.sqrt(HD)


def dot(a, b, dims):
    return lax.dot_general(a, b, dims, preferred_element_type=F32)


def probs_of(key, query, keep):
    scores = dot(key, query, TN) * SCALE
    if keep is not None:
        scores = jnp.where(keep, scores, -jnp.inf)
    top = jnp.max(scores, axis=0, keepdims=True)
    e = jnp.exp(scores - top)
    return e / jnp.sum(e, axis=0, keepdims=True)


def same_position():
    i = lax.broadcasted_iota(jnp.int32, (TOK, TOK), 0)
    j = lax.broadcasted_iota(jnp.int32, (TOK, TOK), 1)
    return ((i + j) & 1) == 0


def turned(x):
    return x.astype(F32).T.astype(BF16)


def rows_of(ref, h):
    return ref[h * HD : (h + 1) * HD, :]


def flat(ref):
    x = ref[...]
    return x.reshape(TOK, x.shape[-1])


def forward_kernel(over_time, q_ref, k_ref, v_ref, out_ref, *turned_refs):
    keep = same_position() if over_time else None
    if over_time:
        for src, dst in zip((q_ref, k_ref, v_ref), turned_refs):
            dst[...] = turned(src[...])
        q_ref, k_ref, v_ref = turned_refs
    for h in range(HEADS):
        low = probs_of(rows_of(k_ref, h), rows_of(q_ref, h), keep).astype(BF16)
        out_ref[h * HD : (h + 1) * HD, :] = dot(rows_of(v_ref, h), low, NN).astype(BF16)


def project_kernel(cot_ref, gate_ref, w_ref, att_ref, d_ref, part_ref):
    cot = flat(cot_ref).astype(F32)
    gated = (cot * gate_ref[...]).astype(BF16)
    d_ref[...] = dot(w_ref[...], gated, NT).astype(BF16)
    projected = dot(att_ref[...], w_ref[...], TN)
    part_ref[...] = jnp.sum(cot * projected, axis=0, keepdims=True)


def backward_kernel(over_time, q_ref, k_ref, v_ref, att_ref, d_ref, gq_ref, gk_ref, gv_ref, *scratch):
    keep = same_position() if over_time else None
    outs = (gq_ref, gk_ref, gv_ref)
    if over_time:
        for src, dst in zip((q_ref, k_ref, v_ref), scratch):
            dst[...] = turned(flat(src))
        q_ref, k_ref, v_ref = scratch[:3]
        outs = scratch[3:]
    for h in range(HEADS):
        sl = slice(h * HD, (h + 1) * HD)
        q, k, v, a, d = (rows_of(r, h) for r in (q_ref, k_ref, v_ref, att_ref, d_ref))
        probs = probs_of(k, q, keep)
        low = probs.astype(BF16)
        d_probs = dot(v, d, TN)
        delta = jnp.sum(d.astype(F32) * a.astype(F32), axis=0, keepdims=True)
        d_scores = (probs * (d_probs - delta)).astype(BF16)
        grads = (dot(k, d_scores, NN) * SCALE, dot(q, d_scores, NT) * SCALE, dot(d, low, NT))
        for ref, g in zip(outs, grads):
            ref[sl, :] = g.astype(ref.dtype)
    if over_time:
        for src, dst in zip(outs, (gq_ref, gk_ref, gv_ref)):
            dst[...] = src[...].T.astype(BF16).reshape(dst.shape)


def select_kernel(core_ref, own_ref, other_ref, gate_ref, out_ref):
    core = core_ref[0]
    row = lax.broadcasted_iota(jnp.int32, (WIDTH, 1), 0)
    block = (row * 3641) >> 16
    channel = row + 18 * (block + core)
    col = lax.broadcasted_iota(jnp.int32, (WIDTH, MODEL), 1)
    pick = jnp.where(col == channel, 1.0, 0.0).astype(BF16)
    for i, ref in enumerate((own_ref, other_ref)):
        gated = (flat(ref).astype(F32) * gate_ref[...]).astype(BF16)
        out_ref[:, i * TOK : (i + 1) * TOK] = dot(pick, gated, NT).astype(BF16)


def packed_block(block):
    tiles = [block[:, 128 * t : 128 * t + 128] for t in range(4)]
    last = jnp.concatenate([block[:18, 512:], block[18:, 512:]], axis=1)
    return jnp.concatenate(tiles + [last], axis=0)


def product_kernel(norm, half_ref, side_ref, own_ref, other_ref, sel_ref, keep_ref, x_ref, y_ref, d_ref):
    first_y = half_ref[0] == 0
    first_x = side_ref[0] == 0
    att = jnp.concatenate([own_ref[...], other_ref[...]], axis=1)
    term = dot(att, sel_ref[...], NT) * norm
    for g in range(4):
        at = [288 * x + HD * g + 36 * y for x in (0, 1) for y in (0, 1)]
        b00, b01, b10, b11 = (packed_block(term[i : i + 36]) for i in at)
        mine = (jnp.where(first_x, b00, b10), jnp.where(first_x, b01, b11))
        theirs = (jnp.where(first_x, b10, b00), jnp.where(first_x, b11, b01))
        keep_ref[g] = jnp.where(first_y, mine[0], mine[1])
        y_ref[g] = jnp.where(first_y, mine[1], mine[0]).astype(BF16)
        x_ref[g] = jnp.where(first_y, theirs[0], theirs[1]).astype(BF16)
        d_ref[g] = jnp.where(first_y, theirs[1], theirs[0]).astype(BF16)


def join_kernel(keep_ref, *rest):
    came, out_ref = rest[:3], rest[3]
    total = keep_ref[...]
    for ref in came:
        total = total + ref[...].astype(F32)
    out_ref[...] = total.astype(BF16)


def pack_kernel(core_ref, in_ref, time_ref, space_ref, came_ref, out_ref):
    total = jnp.sum(in_ref[...].astype(F32), axis=0)
    last = jnp.concatenate([total[144:, :64], total[144:, 64:]], axis=0)
    tiles = [total[36 * t : 36 * t + 36] for t in range(4)]
    total = jnp.concatenate(tiles + [last], axis=1)
    total = jnp.concatenate([total, jnp.zeros((4, WIDTH), F32)], axis=0)
    gate = jnp.where(core_ref[0] == 0, time_ref[...], space_ref[...]) + came_ref[...]
    last = gate[:, 1024:]
    tail = jnp.concatenate([last[:, 16 * a : 16 * a + 16] for a in range(8)], axis=0)
    gap = jnp.zeros((8, 22), F32)
    low = jnp.concatenate([gate[:, 128 * a : 128 * a + 128] for a in range(8)], axis=0)
    for m in range(32):
        parts = [total[8 * b : 8 * b + 8, 18 * m : 18 * m + 18] for b in range(5)]
        high = jnp.concatenate(parts + [gap, tail], axis=1)
        out_ref[m] = jnp.concatenate([high, low], axis=0).astype(BF16)


def finish_kernel(norm, in_ref, out_ref, gate_ref):
    total = jnp.sum(in_ref[...].astype(F32), axis=0)
    high = total[:8]
    flipped = high.T
    for b in range(5):
        n = 8 if b < 4 else 4
        out_ref[:, 8 * b : 8 * b + n] = flipped[18 * b : 18 * b + 18, :n]
    for a in range(8):
        gate_ref[:, 128 * a : 128 * a + 128] = total[8 + a : 9 + a, :] * norm
    last = jnp.concatenate([high[a : a + 1, 112:] for a in range(8)], axis=1)
    gate_ref[:, 1024:] = last * norm


def call(kernel, outs, *args, scratch=(), flops=0, scalars=0):
    specs = [pl.BlockSpec(memory_space=pltpu.SMEM)] * scalars
    specs += [pl.BlockSpec(memory_space=pltpu.VMEM)] * (len(args) - scalars)
    shapes = tuple(jax.ShapeDtypeStruct(s, d) for s, d in outs)
    return pl.pallas_call(
        kernel,
        out_shape=shapes,
        in_specs=specs,
        out_specs=tuple(pl.BlockSpec(memory_space=pltpu.VMEM) for _ in shapes),
        scratch_shapes=list(scratch),
        cost_estimate=pl.CostEstimate(flops=flops, bytes_accessed=1 << 20, transcendentals=0),
        compiler_params=pltpu.CompilerParams(vmem_limit_bytes=VMEM_LIMIT),
    )(*args)


def traded(x, axes):
    return lax.all_to_all(x, axes, 0, 0, tiled=True)


def partner(x, axis):
    return lax.ppermute(x, axis, [(0, 1), (1, 0)])


def swapped(x):
    return jnp.swapaxes(x[0, 0], 0, 1)


US = 400_000_000
VMEM_LIMIT = 16 << 20


def step(cot, qt, kt, vt, qs, ks, vs, wt, ws, gt, gs):
    norm_weight = 1.0 / math.sqrt(16 * 64 * 128)
    norm_gate = 1.0 / math.sqrt(64 * 128)
    col = ((WIDTH, TOK), BF16)
    core = lax.axis_index("c").astype(jnp.int32).reshape(1)
    half = lax.axis_index("yl").astype(jnp.int32).reshape(1)
    side = lax.axis_index("xl").astype(jnp.int32).reshape(1)
    exchanged = traded(cot[0], SEQ)
    other_cot = partner(cot, "c")
    cot_t = cot[0]
    wt_t = wt.T
    ws_t = ws.T
    turned_in = [pltpu.VMEM((WIDTH, TOK), BF16)] * 3
    q2, k2, v2 = (x.reshape(TOK, WIDTH) for x in (qt, kt, vt))
    (att_t,) = call(functools.partial(forward_kernel, True), [col], q2, k2, v2, scratch=turned_in, flops=4 * US)
    other_att = partner(att_t, "c")
    (selected,) = call(select_kernel, [((WIDTH, 2 * TOK), BF16)], core, cot_t, other_cot[0], gt, scalars=1, flops=2 * US)
    block = (4, 162, 128)
    keep, to_x, to_y, to_d = call(functools.partial(product_kernel, norm_weight), [(block, F32)] + [(block, BF16)] * 3, half, side, att_t, other_att, selected, scalars=2, flops=2 * US)
    came_d = lax.ppermute(to_d, ("xl", "yl"), [(i, 3 - i) for i in range(4)])
    came_x = partner(to_x, "xl")
    came_y = partner(to_y, "yl")
    (terms,) = call(join_kernel, [(block, BF16)], keep, came_x, came_y, came_d, flops=US)
    arrived = traded(terms, "yh")
    part = ((1, MODEL), F32)
    d_t, part_t = call(project_kernel, [col, part], cot_t, gt, wt_t, att_t, flops=2 * US)
    q_s, k_s, v_s = (swapped(x) for x in (qs, ks, vs))
    (att_s,) = call(functools.partial(forward_kernel, False), [col], q_s, k_s, v_s, flops=3 * US)
    d_s, part_s = call(project_kernel, [col, part], exchanged, gs, ws_t, att_s, flops=2 * US)
    came_gate = partner(jnp.where(core == 0, part_s, part_t), "c")
    (packed,) = call(pack_kernel, [((32, 16, 128), BF16)], core, arrived, part_t, part_s, came_gate, scalars=1, flops=US)
    rows = traded(packed, ROWS)
    tok = ((64, 2, WIDTH), BF16)
    grads_t = call(functools.partial(backward_kernel, True), [tok] * 3, qt[0], kt[0], vt[0], att_t, d_t, scratch=turned_in + [pltpu.VMEM((WIDTH, TOK), F32)] * 3, flops=4 * US)
    grads_s = call(functools.partial(backward_kernel, False), [col] * 3, q_s, k_s, v_s, att_s, d_s, flops=4 * US)
    weight_grad, gate = call(functools.partial(finish_kernel, norm_gate), [((18, 36), F32), part], rows, flops=US)
    other_gate = partner(gate, "c")
    return (
        *(g[None] for g in grads_t),
        *(jnp.swapaxes(g, 0, 1)[None, None] for g in grads_s),
        weight_grad,
        jnp.where(core == 0, gate, other_gate),
        jnp.where(core == 0, other_gate, gate),
    )


def solution(mesh):
    fine = Mesh(np.array(mesh.devices).reshape(2, 4, 2, 16, 2, 2), ("xl", "yh", "yl", "z", "xh", "c"))
    by_pos = P(DP, None, SEQ, None)
    by_frame = P(DP, SEQ, None, None)
    in_specs = (by_pos,) * 4 + (by_frame,) * 3 + (P(), P(), P(DP, None), P(DP, None))
    out_specs = (by_pos,) * 3 + (by_frame,) * 3 + (P(SEQ, DP), P(DP, None), P(DP, None))
    return jax.shard_map(step, mesh=fine, in_specs=in_specs, out_specs=out_specs, check_vma=False)
```
